512 devices in a mesh: section: 32 (over x, y_hi, core), dp: 16 (over y_lo, z).
Axes of the slice: x: 4, y: 8 (y_hi: 4, y_lo: 2; y = y_hi * 2 + y_lo), z: 8, core: 2. Of those that a mesh axis runs over, the one named last changes fastest.
Arguments:
- out_pair: float32 [2048, 2048], P('dp'), may hold values from -6 to 6
- out_grad: bfloat16 [2048, 2048], P('dp'), may hold values from -6 to 6
- f_weight: bfloat16 [32, 1024, 1024], P('section', 'dp'), may hold values from -0.09375 to 0.09375
- g_weight: bfloat16 [32, 1024, 1024], P('section', 'dp'), may hold values from -0.09375 to 0.09375
- gains: float32 [32, 2, 1024], P('section'), may hold values from 0.1 to 1.9
Outputs:
- in_pair: float32 [32, 2048, 2048], P('section', 'dp')
- in_grad: bfloat16 [32, 2048, 2048], P('section', 'dp')
- f_grad: float32 [32, 1024, 1024], P('section', 'dp')
- g_grad: float32 [32, 1024, 1024], P('section', 'dp')
- gains_grad: float32 [32, 2, 1024], P('section')
The draws below stay inside these ranges and needn't reach their ends.
All inputs are finite; a program needn't handle non-finite values.
Results may differ from the reference program's by a relative error of at most 0.04.
Values may be sent and summed in bfloat16 or wider, within the bound.
A program may use at most 64 MiB of HBM per device.

```python
import jax
import jax.numpy as jnp
from jax import lax

DH = 1024
TOK_DEV = 128
SECTIONS = 32
TOKENS = 2048
N_SECTION = 32
N_DP = 16


def steps_of(key, extent, shards, smallest, top_value):
    gain, own = 1.0, jax.random.fold_in(key, 6)
    for dim, parts in shards:
        steps = jnp.exp(jax.random.uniform(jax.random.fold_in(own, dim), (parts,), jnp.float32, smallest / len(shards), top_value / len(shards)))
        gain = gain * jnp.repeat(steps, extent[dim] // parts).reshape([-1 if axis == dim else 1 for axis in range(len(extent))])
    return gain


def centred(key, dims, width, reach, shards=(), kind=jnp.bfloat16):
    result = width * jax.random.normal(key, dims, jnp.float32)
    if shards:
        result = result * steps_of(key, dims, shards, -0.22, 0.18)
    return jnp.clip(result, -reach, reach).astype(kind)


def setup_inputs(seed: int = 0) -> dict:
    seeds = jax.random.split(jax.random.key(seed), 6)
    out_pair = centred(seeds[0], (TOKENS, 2 * DH), 1.0, 6.0, ((0, 16),), jnp.float32)
    out_grad = centred(seeds[1], (TOKENS, 2 * DH), 1.0, 6.0, ((0, 16),))
    f_weight = centred(seeds[2], (SECTIONS, DH, DH), (4 * DH) ** -0.5, 0.09375, ((0, 32), (1, 16)))
    g_weight = centred(seeds[3], (SECTIONS, DH, DH), (4 * DH) ** -0.5, 0.09375, ((0, 32), (1, 16)))
    gains = jnp.clip(1.0 + 0.18 * jax.random.normal(seeds[4], (SECTIONS, 2, DH), jnp.float32), 0.1, 1.9)
    return {"out_pair": out_pair, "out_grad": out_grad, "f_weight": f_weight, "g_weight": g_weight, "gains": gains}


offset = 0.25

def silu_parts(pre_values):
    sigmoid_value = jax.nn.sigmoid(pre_values)
    return (pre_values * sigmoid_value, sigmoid_value * (1.0 + pre_values * (1.0 - sigmoid_value)))

def normalize(values, gain_row):
    inv_scale = lax.rsqrt(lax.optimization_barrier(jnp.mean(values * values, axis=-1, keepdims=True)) + offset)
    return ((values * inv_scale * gain_row).astype(jnp.bfloat16), inv_scale)

def norm_back(values, inv_scale, gain_row, upstream):
    weighted = gain_row * upstream
    cubed = inv_scale * inv_scale * inv_scale
    return inv_scale * weighted - values * cubed * lax.optimization_barrier(jnp.mean(weighted * values, axis=-1, keepdims=True))

def coupling_back(upper_out, lower_out, upper_grad, lower_grad, w_first, w_second, gain_pair):
    normed_second, scale_second = normalize(upper_out, gain_pair[1])
    pre_second = jnp.dot(normed_second, w_second, preferred_element_type=jnp.float32)
    act_second, slope_second = silu_parts(pre_second)
    lower_in = lower_out - act_second
    normed_first, scale_first = normalize(lower_in, gain_pair[0])
    pre_first = jnp.dot(normed_first, w_first, preferred_element_type=jnp.float32)
    act_first, slope_first = silu_parts(pre_first)
    upper_in = upper_out - act_first
    delta_second = (lower_grad * slope_second).astype(jnp.bfloat16)
    back_second = jnp.dot(delta_second, w_second.T, preferred_element_type=jnp.float32)
    through = upper_grad + norm_back(upper_out, scale_second, gain_pair[1], back_second)
    delta_first = (through * slope_first).astype(jnp.bfloat16)
    back_first = jnp.dot(delta_first, w_first.T, preferred_element_type=jnp.float32)
    lower_total = lower_grad + norm_back(lower_in, scale_first, gain_pair[0], back_first)
    gain_terms = jnp.stack([lax.optimization_barrier(jnp.sum(back_first * lower_in * scale_first, axis=0)), lax.optimization_barrier(jnp.sum(back_second * upper_out * scale_second, axis=0))])
    return (upper_in, lower_in, through.astype(jnp.bfloat16), lower_total.astype(jnp.bfloat16), normed_first, delta_first, normed_second, delta_second, gain_terms)

def replica_sum(normed, delta):
    left_side = normed.reshape(N_DP, TOK_DEV, -1).astype(jnp.float32)
    right_side = delta.reshape(N_DP, TOK_DEV, -1).astype(jnp.float32)
    partial_sums = jnp.einsum('rtd,rte->rde', left_side, right_side)
    rounded = lax.optimization_barrier(partial_sums.astype(jnp.bfloat16))
    return lax.optimization_barrier(jnp.sum(rounded.astype(jnp.float32), axis=0))

def reference(out_pair, out_grad, f_weight, g_weight, gains):
    channels = out_pair.shape[1] // 2
    pair_now = out_pair
    grad_now = out_grad
    pairs, grads, first_sums, second_sums, gain_sums = ([], [], [], [], [])
    for layer_index in range(N_SECTION - 1, -1, -1):
        results = coupling_back(pair_now[:, :channels], pair_now[:, channels:], grad_now[:, :channels].astype(jnp.float32), grad_now[:, channels:].astype(jnp.float32), f_weight[layer_index], g_weight[layer_index], gains[layer_index])
        pair_now = jnp.concatenate([results[0], results[1]], axis=1)
        grad_now = jnp.concatenate([results[2], results[3]], axis=1)
        pairs.append(pair_now)
        grads.append(grad_now)
        first_sums.append(replica_sum(results[4], results[5]))
        second_sums.append(replica_sum(results[6], results[7]))
        gain_sums.append(results[8])
    return (jnp.stack(pairs[::-1]), jnp.stack(grads[::-1]), jnp.stack(first_sums[::-1]), jnp.stack(second_sums[::-1]), jnp.stack(gain_sums[::-1]))
```

```python
import functools

import jax
import jax.numpy as jnp
from jax import lax
from jax.experimental import pallas as pl
from jax.experimental.pallas import tpu as pltpu
from jax.sharding import PartitionSpec as P

MESH = pl.DeviceIdType.MESH
BF = jnp.bfloat16
F32 = jnp.float32
OFFSET = 0.25
NY = 2
ROWS = 16


def arrived(ref, sem):
    pltpu.make_async_copy(ref, ref, sem).wait()


def relay_kernel(
    n_section, n_dp, top_pair, top_grad, f_own, g_own, gains_own,
    pair_out, grad_out, part_out, gain_out,
    W, gain, ract, rgrad, nbuf, obuf, xbuf, rbuf, dbuf, gbuf, gacc, gsum,
    s_own, w_recv, w_peer, s_d2d, s_y, s_z, s_gain,
    s_ract, s_next, s_rgrad, s_gnext, s_x, r_x, s_r, r_r, s_pair, r_pair, s_d, r_d, s_grad, r_grad, s_gs,
):
    section = lax.axis_index("section")
    dp = lax.axis_index("dp")
    core = lax.rem(section, 2)
    chip = section // 2
    chips = n_section // 2
    nz = n_dp // NY
    half = nz // 2
    y, z = dp // nz, lax.rem(dp, nz)
    slab, dh = f_own.shape[1], f_own.shape[2]
    tok = ract.shape[0]
    blocks = tok // ROWS
    first = chip == chips - 1
    last = chip == 0
    partner = {"section": section + 1 - 2 * core}
    y_peer = {"dp": (1 - y) * nz + z}

    def z_peer(sign):
        return {"dp": y * nz + lax.rem(z + sign + nz, nz)}

    def remote(src, dst, send, recv, where):
        return pltpu.make_async_remote_copy(
            src_ref=src, dst_ref=dst, send_sem=send, recv_sem=recv, device_id=where, device_id_type=MESH
        )

    barrier = pltpu.get_barrier_semaphore()
    for where in (partner, y_peer, z_peer(1), z_peer(-1)):
        pl.semaphore_signal(barrier, inc=1, device_id=where, device_id_type=MESH)

    @pl.when(chip < chips - 1)
    def _():
        pl.semaphore_signal(barrier, inc=1, device_id={"section": section + 2}, device_id_type=MESH)

    @pl.when(chip > 0)
    def _():
        pl.semaphore_signal(barrier, inc=1, device_id={"section": section - 2}, device_id_type=MESH)

    own_f = pltpu.make_async_copy(f_own.at[0], W.at[core, 0, pl.ds(dp * slab, slab), :], s_own.at[0])
    own_g = pltpu.make_async_copy(g_own.at[0], W.at[core, 1, pl.ds(dp * slab, slab), :], s_own.at[1])
    own_c = pltpu.make_async_copy(gains_own.at[0], gain.at[core], s_own.at[2])
    own_g.start()
    own_f.start()
    own_c.start()
    gacc[...] = jnp.zeros_like(gacc)
    pl.semaphore_wait(barrier, 4 + jnp.where(chip < chips - 1, 1, 0) + jnp.where(chip > 0, 1, 0))

    def top_copy(b, part, src, dst, sem):
        rows, cols = pl.ds(b * ROWS, ROWS), pl.ds(part * dh, dh)
        return pltpu.make_async_copy(src.at[rows, cols], dst.at[rows, cols], sem.at[b, part])

    @pl.when(jnp.logical_and(first, core == 1))
    def _():
        def go(b, _):
            top_copy(b, 0, top_pair, ract, s_ract).start()
            top_copy(b, 1, top_pair, ract, s_ract).start()
            return 0
        lax.fori_loop(0, blocks, go, 0)

    @pl.when(jnp.logical_and(first, core == 0))
    def _():
        def go(b, _):
            top_copy(b, 0, top_grad, rgrad, s_rgrad).start()
            top_copy(b, 1, top_grad, rgrad, s_rgrad).start()
            return 0
        lax.fori_loop(0, blocks, go, 0)

    def index_of(plane, zz):
        return plane * nz + lax.rem(zz + nz, nz)

    def item(h, index):
        return W.at[core, h, pl.ds(index * slab, slab), :]

    def to_peer(h, index):
        return remote(item(h, index), item(h, index), s_d2d.at[h, index], w_peer.at[h, index], partner)

    def to_y(h, index):
        return remote(item(h, index), item(h, index), s_y.at[h, index], w_recv.at[h, index], y_peer)

    CHAINS = ((1, 0), (1, 1), (0, 0))

    def to_z(chain, direction, step, sign):
        h, other = CHAINS[chain]
        plane = y if other == 0 else 1 - y
        index = index_of(plane, z - sign * step)
        return remote(item(h, index), item(h, index), s_z.at[chain, direction, step], w_recv.at[h, index], z_peer(sign))

    long_sign = 1 - 2 * core

    def sends(chain, step):
        if step < half - 1:
            return [to_z(chain, 0, step, 1), to_z(chain, 1, step, -1)]
        return [to_z(chain, 0, step, long_sign)]

    own_g.wait()
    to_y(1, dp).start()
    for copy in sends(0, 0):
        copy.start()
    own_f.wait()
    for copy in sends(2, 0):
        copy.start()
    to_y(0, dp).start()
    to_peer(1, dp).start()
    to_peer(0, dp).start()
    own_c.wait()
    gain_copy = remote(gain.at[core], gain.at[core], s_gain.at[0], s_gain.at[1], partner)
    gain_copy.start()
    other_own = index_of(1 - y, z)
    arrived(item(1, other_own), w_recv.at[1, other_own])
    for copy in sends(1, 0):
        copy.start()
    to_peer(1, other_own).start()
    for step in range(1, half + 1):
        for chain in (0, 1, 2):
            h, other = CHAINS[chain]
            plane = y if other == 0 else 1 - y
            for sign in (1, -1) if step < half else (1,):
                index = index_of(plane, z - sign * step)
                arrived(item(h, index), w_recv.at[h, index])
                if step < half - 1:
                    to_z(chain, 0 if sign == 1 else 1, step, sign).start()
                to_peer(h, index).start()
                if h == 0:
                    to_y(0, index).start()
            if step == half - 1:
                for copy in sends(chain, step):
                    copy.start()
    for zz in range(nz):
        index = index_of(1 - y, z + zz)
        arrived(item(0, index), w_recv.at[0, index])
        to_peer(0, index).start()

    def peer_item(h, index):
        return W.at[1 - core, h, pl.ds(index * slab, slab), :]

    def peer_wait(index, _):
        for h in (1, 0):
            arrived(peer_item(h, index), w_peer.at[h, index])
        return 0

    lax.fori_loop(0, n_dp, peer_wait, 0)
    arrived(gain.at[1 - core], s_gain.at[1])

    def rows_of(b):
        return pl.ds(pl.multiple_of(b * ROWS, ROWS), ROWS)

    def next_copy(b, part):
        rows, cols = rows_of(b), pl.ds(part * dh, dh)
        return remote(nbuf.at[rows, cols], ract.at[rows, cols], s_next.at[b, part], s_ract.at[b, part], {"section": section - 2})

    def gnext_copy(b, part):
        rows, cols = rows_of(b), pl.ds(part * dh, dh)
        return remote(gbuf.at[0, rows, cols], rgrad.at[rows, cols], s_gnext.at[b, part], s_rgrad.at[b, part], {"section": section - 2})

    def x_copy(lay, b):
        at = xbuf.at[lay, :, rows_of(b), :]
        return remote(at, at, s_x.at[lay, b], r_x.at[lay, b], partner)

    def r_copy(lay, b):
        at = rbuf.at[lay, :, rows_of(b), :]
        return remote(at, at, s_r.at[lay, b], r_r.at[lay, b], partner)

    def d_copy(b):
        at = dbuf.at[1, :, rows_of(b), :]
        return remote(at, at, s_d.at[b], r_d.at[b], partner)

    def pair_copy(lay, b):
        src, dst = obuf.at[lay, rows_of(b), :], pair_out.at[0, rows_of(b), :]
        if lay == 1:
            return pltpu.make_async_copy(src, dst, s_pair.at[lay, b])
        return remote(src, dst, s_pair.at[lay, b], r_pair.at[b], partner)

    def grad_copy(lay, b):
        src, dst = gbuf.at[lay, rows_of(b), :], grad_out.at[0, rows_of(b), :]
        if lay == 0:
            return pltpu.make_async_copy(src, dst, s_grad.at[lay, b])
        return remote(src, dst, s_grad.at[lay, b], r_grad.at[b], partner)

    def sent(copy, is_local):
        if is_local:
            copy.wait()
        else:
            copy.wait_send()

    @pl.when(core == 1)
    def _():
        def act(b, _):
            rows = rows_of(b)
            for part in (1, 0):
                cols = pl.ds(part * dh, dh)
                arrived(ract.at[rows, cols], s_ract.at[b, part])
            y1 = ract[rows, :dh].astype(F32)
            y2 = ract[rows, dh:].astype(F32)
            for lay in (1, 0):
                cf, cg = gain[lay, 0:1, :], gain[lay, 1:2, :]
                rg = lax.rsqrt(jnp.mean(y1 * y1, axis=-1, keepdims=True) + OFFSET)
                ug = y1 * rg
                pre = jnp.dot((ug * cg).astype(BF), W[lay, 1], preferred_element_type=F32)
                sig = jax.nn.sigmoid(pre)
                silu = pre * sig
                x2 = y2 - silu
                sg = sig + silu * (1.0 - sig)
                obuf[lay, rows, dh:] = x2
                if lay == 0:
                    nbuf[rows, dh:] = x2.astype(BF)

                    @pl.when(jnp.logical_not(last))
                    def _():
                        next_copy(b, 1).start()
                rf = lax.rsqrt(jnp.mean(x2 * x2, axis=-1, keepdims=True) + OFFSET)
                uf = x2 * rf
                pre = jnp.dot((uf * cf).astype(BF), W[lay, 0], preferred_element_type=F32)
                sig = jax.nn.sigmoid(pre)
                silu = pre * sig
                x1 = y1 - silu
                sf = sig + silu * (1.0 - sig)
                if lay == 0:
                    nbuf[rows, :dh] = x1.astype(BF)

                    @pl.when(jnp.logical_not(last))
                    def _():
                        next_copy(b, 0).start()
                obuf[lay, rows, :dh] = x1
                xbuf[lay, 0, rows, :] = uf.astype(BF)
                xbuf[lay, 1, rows, :] = ug.astype(BF)
                xbuf[lay, 2, rows, :] = sf.astype(BF)
                xbuf[lay, 3, rows, :] = sg.astype(BF)
                rbuf[lay, 0, rows, :] = jnp.broadcast_to(rf, (ROWS, 128))
                rbuf[lay, 1, rows, :] = jnp.broadcast_to(rg, (ROWS, 128))
                x_copy(lay, b).start()
                r_copy(lay, b).start()
                pair_copy(lay, b).start()
                y1, y2 = x1, x2
            return 0

        lax.fori_loop(0, blocks, act, 0)

    def times_transposed(delta, weight):
        return lax.dot_general(delta, weight, (((1,), (1,)), ((), ())), preferred_element_type=F32)

    @pl.when(core == 0)
    def _():
        def grad(b, _):
            rows = rows_of(b)
            for part in (0, 1):
                cols = pl.ds(part * dh, dh)
                arrived(rgrad.at[rows, cols], s_rgrad.at[b, part])
            gy1 = rgrad[rows, :dh].astype(F32)
            gy2 = rgrad[rows, dh:].astype(F32)
            for lay in (1, 0):
                arrived(xbuf.at[lay, :, rows, :], r_x.at[lay, b])
                arrived(rbuf.at[lay, :, rows, :], r_r.at[lay, b])
                cf, cg = gain[lay, 0:1, :], gain[lay, 1:2, :]
                uf, ug = xbuf[lay, 0, rows, :].astype(F32), xbuf[lay, 1, rows, :].astype(F32)
                sf, sg = xbuf[lay, 2, rows, :].astype(F32), xbuf[lay, 3, rows, :].astype(F32)
                rf, rg = rbuf[lay, 0, rows, 0:1], rbuf[lay, 1, rows, 0:1]
                delta = (gy2 * sg).astype(BF)
                dbuf[lay, 1, rows, :] = delta
                back = times_transposed(delta, W[lay, 1])
                gacc[lay, 1] += back * ug
                w = cg * back
                gz = gy1 + rg * (w - ug * jnp.mean(w * ug, axis=-1, keepdims=True))
                gbuf[lay, rows, :dh] = gz.astype(BF)
                if lay == 0:
                    @pl.when(jnp.logical_not(last))
                    def _():
                        gnext_copy(b, 0).start()
                delta = (gz * sf).astype(BF)
                dbuf[lay, 0, rows, :] = delta
                back = times_transposed(delta, W[lay, 0])
                gacc[lay, 0] += back * uf
                w = cf * back
                gx = gy2 + rf * (w - uf * jnp.mean(w * uf, axis=-1, keepdims=True))
                gbuf[lay, rows, dh:] = gx.astype(BF)
                if lay == 0:
                    @pl.when(jnp.logical_not(last))
                    def _():
                        gnext_copy(b, 1).start()
                else:
                    d_copy(b).start()
                grad_copy(lay, b).start()
                gy1, gy2 = gz, gx
            return 0

        lax.fori_loop(0, blocks, grad, 0)
        for lay in (0, 1):
            gsum[lay] = jnp.sum(gacc[lay], axis=1)
        remote(gsum.at[1], gsum.at[1], s_gs.at[0], s_gs.at[1], partner).start()

    @pl.when(core == 1)
    def _():
        def wait_d(b, _):
            arrived(dbuf.at[1, :, rows_of(b), :], r_d.at[b])
            return 0
        lax.fori_loop(0, blocks, wait_d, 0)
        arrived(gsum.at[1], s_gs.at[1])

    gain_out[0] = gsum[core]
    width = min(128, dh)

    def outer(i, _):
        at = pl.ds(pl.multiple_of(i * width, width), width)
        for h in (0, 1):
            normed = (xbuf[core, h, :, at].astype(F32) * gain[core, h, at][None, :]).astype(BF)
            part = lax.dot_general(normed, dbuf[core, h], (((0,), (0,)), ((), ())), preferred_element_type=F32)
            part_out[at, h * dh:(h + 1) * dh] = part.astype(BF)
        return 0

    lax.fori_loop(0, dh // width, outer, 0)

    @pl.when(core == 1)
    def _():
        def done(b, _):
            for lay in (0, 1):
                x_copy(lay, b).wait_send()
                r_copy(lay, b).wait_send()
                sent(pair_copy(lay, b), lay == 1)
            arrived(grad_out.at[0, rows_of(b), :], r_grad.at[b])

            @pl.when(jnp.logical_not(last))
            def _():
                next_copy(b, 0).wait_send()
                next_copy(b, 1).wait_send()
            return 0
        lax.fori_loop(0, blocks, done, 0)

    @pl.when(core == 0)
    def _():
        def done(b, _):
            d_copy(b).wait_send()
            for lay in (0, 1):
                sent(grad_copy(lay, b), lay == 0)
            arrived(pair_out.at[0, rows_of(b), :], r_pair.at[b])

            @pl.when(jnp.logical_not(last))
            def _():
                gnext_copy(b, 0).wait_send()
                gnext_copy(b, 1).wait_send()
            return 0
        lax.fori_loop(0, blocks, done, 0)
        remote(gsum.at[1], gsum.at[1], s_gs.at[0], s_gs.at[1], partner).wait_send()

    gain_copy.wait_send()
    to_y(1, dp).wait_send()

    def y_done(zz, _):
        to_y(0, index_of(y, zz)).wait_send()
        return 0
    lax.fori_loop(0, nz, y_done, 0)

    def peer_done(index, _):
        to_peer(0, index).wait_send()
        to_peer(1, index).wait_send()
        return 0
    lax.fori_loop(0, n_dp, peer_done, 0)
    for chain in (0, 1, 2):
        for step in range(half):
            for copy in sends(chain, step):
                copy.wait_send()


def shards(n_section, n_dp, out_pair, out_grad, f_weight, g_weight, gains):
    tok, width = out_pair.shape
    dh = width // 2
    slab = f_weight.shape[1]
    blocks = tok // ROWS
    nz = n_dp // NY
    half = nz // 2
    any_space = pl.BlockSpec(memory_space=pl.ANY)
    vmem = pl.BlockSpec(memory_space=pltpu.VMEM)
    dma = pltpu.SemaphoreType.DMA
    pair, grad, part, gain = pl.pallas_call(
        functools.partial(relay_kernel, n_section, n_dp),
        out_shape=(
            jax.ShapeDtypeStruct((1, tok, width), F32),
            jax.ShapeDtypeStruct((1, tok, width), BF),
            jax.ShapeDtypeStruct((dh, width), BF),
            jax.ShapeDtypeStruct((1, 2, dh), F32),
        ),
        in_specs=[any_space] * 5,
        out_specs=(any_space, any_space, vmem, vmem),
        scratch_shapes=[
            pltpu.VMEM((2, 2, dh, dh), BF),
            pltpu.VMEM((2, 2, dh), F32),
            pltpu.VMEM((tok, width), BF),
            pltpu.VMEM((tok, width), BF),
            pltpu.VMEM((tok, width), BF),
            pltpu.VMEM((2, tok, width), F32),
            pltpu.VMEM((2, 4, tok, dh), BF),
            pltpu.VMEM((2, 2, tok, 128), F32),
            pltpu.VMEM((2, 2, tok, dh), BF),
            pltpu.VMEM((2, tok, width), BF),
            pltpu.VMEM((2, 2, ROWS, dh), F32),
            pltpu.VMEM((2, 2, dh), F32),
            dma((3,)), dma((2, n_dp)), dma((2, n_dp)), dma((2, n_dp)), dma((2, n_dp)), dma((3, 2, half)), dma((2,)),
            dma((blocks, 2)), dma((blocks, 2)), dma((blocks, 2)), dma((blocks, 2)),
            dma((2, blocks)), dma((2, blocks)), dma((2, blocks)), dma((2, blocks)),
            dma((2, blocks)), dma((blocks,)), dma((blocks,)), dma((blocks,)), dma((2, blocks)), dma((blocks,)), dma((2,)),
        ],
        compiler_params=pltpu.CompilerParams(
            collective_id=0, has_side_effects=True, vmem_limit_bytes=60 * 1024 * 1024
        ),
        name="relay",
    )(out_pair.astype(BF), out_grad, f_weight, g_weight, gains)
    summed = lax.psum_scatter(part, "dp", scatter_dimension=0, tiled=True).astype(F32)
    gain = lax.psum(gain, "dp")
    return pair, grad, summed[None, :, :dh], summed[None, :, dh:], gain


def solution(mesh):
    sizes = dict(mesh.shape)
    return jax.shard_map(
        functools.partial(shards, sizes["section"], sizes["dp"]),
        mesh=mesh,
        in_specs=(P("dp", None), P("dp", None), P("section", "dp", None), P("section", "dp", None), P("section", None, None)),
        out_specs=(
            P("section", "dp", None),
            P("section", "dp", None),
            P("section", "dp", None),
            P("section", "dp", None),
            P("section", None, None),
        ),
        check_vma=False,
    )
```

```python
import functools

import jax
import jax.numpy as jnp
from jax import lax
from jax.experimental import pallas as pl
from jax.experimental.pallas import tpu as pltpu
from jax.sharding import PartitionSpec as P

MESH = pl.DeviceIdType.MESH
BF = jnp.bfloat16
F32 = jnp.float32
OFFSET = 0.25
NY = 2
ROWS = 16


def arrived(ref, sem):
    pltpu.make_async_copy(ref, ref, sem).wait()


def relay_kernel(
    n_section, n_dp, top_pair, top_grad, f_own, g_own, gains_own,
    pair_out, grad_out, f_out, g_out, gain_out,
    W, gain, ract, rgrad, nbuf, obuf, xbuf, rbuf, dbuf, gbuf, gacc, gsum,
    P_, RZ, RY, YG, gslot, gmine, gpeer,
    s_own, w_recv, w_peer, s_d2d, s_y, s_z, s_gain,
    s_ract, s_next, s_rgrad, s_gnext, s_x, r_x, s_r, r_r, s_pair, r_pair, s_d, r_d, s_grad, r_grad, s_gs,
    qs_z, qr_z, qs_y, qr_y, es_z, er_z, es_y,
):
    section = lax.axis_index("section")
    dp = lax.axis_index("dp")
    core = lax.rem(section, 2)
    chip = section // 2
    chips = n_section // 2
    nz = n_dp // NY
    half = nz // 2
    y, z = dp // nz, lax.rem(dp, nz)
    slab, dh = f_own.shape[1], f_own.shape[2]
    tok = ract.shape[0]
    blocks = tok // ROWS
    first = chip == chips - 1
    last = chip == 0
    partner = {"section": section + 1 - 2 * core}
    y_peer = {"dp": (1 - y) * nz + z}

    def z_peer(sign):
        return {"dp": y * nz + lax.rem(z + sign + nz, nz)}

    def remote(src, dst, send, recv, where):
        return pltpu.make_async_remote_copy(
            src_ref=src, dst_ref=dst, send_sem=send, recv_sem=recv, device_id=where, device_id_type=MESH
        )

    barrier = pltpu.get_barrier_semaphore()
    for where in (partner, y_peer, z_peer(1), z_peer(-1)):
        pl.semaphore_signal(barrier, inc=1, device_id=where, device_id_type=MESH)

    @pl.when(chip < chips - 1)
    def _():
        pl.semaphore_signal(barrier, inc=1, device_id={"section": section + 2}, device_id_type=MESH)

    @pl.when(chip > 0)
    def _():
        pl.semaphore_signal(barrier, inc=1, device_id={"section": section - 2}, device_id_type=MESH)

    own_f = pltpu.make_async_copy(f_own.at[0], W.at[core, 0, pl.ds(dp * slab, slab), :], s_own.at[0])
    own_g = pltpu.make_async_copy(g_own.at[0], W.at[core, 1, pl.ds(dp * slab, slab), :], s_own.at[1])
    own_c = pltpu.make_async_copy(gains_own.at[0], gain.at[core], s_own.at[2])
    own_g.start()
    own_f.start()
    own_c.start()
    gacc[...] = jnp.zeros_like(gacc)
    pl.semaphore_wait(barrier, 4 + jnp.where(chip < chips - 1, 1, 0) + jnp.where(chip > 0, 1, 0))

    def top_copy(b, part, src, dst, sem):
        rows, cols = pl.ds(b * ROWS, ROWS), pl.ds(part * dh, dh)
        return pltpu.make_async_copy(src.at[rows, cols], dst.at[rows, cols], sem.at[b, part])

    @pl.when(jnp.logical_and(first, core == 1))
    def _():
        load = pltpu.make_async_copy(top_pair, obuf.at[0], s_own.at[3])
        load.start()
        load.wait()
        ract[...] = obuf[0].astype(BF)

    @pl.when(jnp.logical_and(first, core == 0))
    def _():
        def go(b, _):
            top_copy(b, 0, top_grad, rgrad, s_rgrad).start()
            top_copy(b, 1, top_grad, rgrad, s_rgrad).start()
            return 0
        lax.fori_loop(0, blocks, go, 0)

    def index_of(plane, zz):
        return plane * nz + lax.rem(zz + nz, nz)

    def item(h, index):
        return W.at[core, h, pl.ds(index * slab, slab), :]

    def to_peer(h, index):
        return remote(item(h, index), item(h, index), s_d2d.at[h, index], w_peer.at[h, index], partner)

    def to_y(h, index):
        return remote(item(h, index), item(h, index), s_y.at[h, index], w_recv.at[h, index], y_peer)

    CHAINS = ((1, 0), (1, 1), (0, 0))

    def to_z(chain, direction, step, sign):
        h, other = CHAINS[chain]
        plane = y if other == 0 else 1 - y
        index = index_of(plane, z - sign * step)
        return remote(item(h, index), item(h, index), s_z.at[chain, direction, step], w_recv.at[h, index], z_peer(sign))

    long_sign = 1 - 2 * core

    def sends(chain, step):
        if step < half - 1:
            return [to_z(chain, 0, step, 1), to_z(chain, 1, step, -1)]
        return [to_z(chain, 0, step, long_sign)]

    own_g.wait()
    to_y(1, dp).start()
    for copy in sends(0, 0):
        copy.start()
    own_f.wait()
    for copy in sends(2, 0):
        copy.start()
    to_y(0, dp).start()
    to_peer(1, dp).start()
    to_peer(0, dp).start()
    own_c.wait()
    gain_copy = remote(gain.at[core], gain.at[core], s_gain.at[0], s_gain.at[1], partner)
    gain_copy.start()
    other_own = index_of(1 - y, z)
    arrived(item(1, other_own), w_recv.at[1, other_own])
    for copy in sends(1, 0):
        copy.start()
    to_peer(1, other_own).start()
    for step in range(1, half + 1):
        for chain in (0, 1, 2):
            h, other = CHAINS[chain]
            plane = y if other == 0 else 1 - y
            for sign in (1, -1) if step < half else (1,):
                index = index_of(plane, z - sign * step)
                arrived(item(h, index), w_recv.at[h, index])
                if step < half - 1:
                    to_z(chain, 0 if sign == 1 else 1, step, sign).start()
                to_peer(h, index).start()
                if h == 0:
                    to_y(0, index).start()
            if step == half - 1:
                for copy in sends(chain, step):
                    copy.start()
    for zz in range(nz):
        index = index_of(1 - y, z + zz)
        arrived(item(0, index), w_recv.at[0, index])
        to_peer(0, index).start()

    def peer_item(h, index):
        return W.at[1 - core, h, pl.ds(index * slab, slab), :]

    def peer_wait(index, _):
        for h in (1, 0):
            arrived(peer_item(h, index), w_peer.at[h, index])
        return 0

    lax.fori_loop(0, n_dp, peer_wait, 0)
    arrived(gain.at[1 - core], s_gain.at[1])

    def rows_of(b):
        return pl.ds(pl.multiple_of(b * ROWS, ROWS), ROWS)

    def next_copy(b, part):
        rows, cols = rows_of(b), pl.ds(part * dh, dh)
        return remote(nbuf.at[rows, cols], ract.at[rows, cols], s_next.at[b, part], s_ract.at[b, part], {"section": section - 2})

    def gnext_copy(b, part):
        rows, cols = rows_of(b), pl.ds(part * dh, dh)
        return remote(gbuf.at[0, rows, cols], rgrad.at[rows, cols], s_gnext.at[b, part], s_rgrad.at[b, part], {"section": section - 2})

    def x_copy(lay, b):
        at = xbuf.at[lay, :, rows_of(b), :]
        return remote(at, at, s_x.at[lay, b], r_x.at[lay, b], partner)

    def r_copy(lay, b):
        at = rbuf.at[lay, :, rows_of(b), :]
        return remote(at, at, s_r.at[lay, b], r_r.at[lay, b], partner)

    def d_copy(b):
        at = dbuf.at[1, :, rows_of(b), :]
        return remote(at, at, s_d.at[b], r_d.at[b], partner)

    def pair_copy(lay, b):
        src, dst = obuf.at[lay, rows_of(b), :], pair_out.at[0, rows_of(b), :]
        if lay == 1:
            return pltpu.make_async_copy(src, dst, s_pair.at[lay, b])
        return remote(src, dst, s_pair.at[lay, b], r_pair.at[b], partner)

    def grad_copy(lay, b):
        src, dst = gbuf.at[lay, rows_of(b), :], grad_out.at[0, rows_of(b), :]
        if lay == 0:
            return pltpu.make_async_copy(src, dst, s_grad.at[lay, b])
        return remote(src, dst, s_grad.at[lay, b], r_grad.at[b], partner)

    def sent(copy, is_local):
        if is_local:
            copy.wait()
        else:
            copy.wait_send()

    @pl.when(core == 1)
    def _():
        def act(b, _):
            rows = rows_of(b)

            @pl.when(jnp.logical_not(first))
            def _():
                for part in (1, 0):
                    cols = pl.ds(part * dh, dh)
                    arrived(ract.at[rows, cols], s_ract.at[b, part])

            y1 = ract[rows, :dh].astype(F32)
            y2 = ract[rows, dh:].astype(F32)
            for lay in (1, 0):
                cf, cg = gain[lay, 0:1, :], gain[lay, 1:2, :]
                rg = lax.rsqrt(jnp.mean(y1 * y1, axis=-1, keepdims=True) + OFFSET)
                ug = y1 * rg
                pre = jnp.dot((ug * cg).astype(BF), W[lay, 1], preferred_element_type=F32)
                sig = jax.nn.sigmoid(pre)
                silu = pre * sig
                x2 = y2 - silu
                sg = sig + silu * (1.0 - sig)
                obuf[lay, rows, dh:] = x2
                if lay == 0:
                    nbuf[rows, dh:] = x2.astype(BF)

                    @pl.when(jnp.logical_not(last))
                    def _():
                        next_copy(b, 1).start()
                rf = lax.rsqrt(jnp.mean(x2 * x2, axis=-1, keepdims=True) + OFFSET)
                uf = x2 * rf
                pre = jnp.dot((uf * cf).astype(BF), W[lay, 0], preferred_element_type=F32)
                sig = jax.nn.sigmoid(pre)
                silu = pre * sig
                x1 = y1 - silu
                sf = sig + silu * (1.0 - sig)
                if lay == 0:
                    nbuf[rows, :dh] = x1.astype(BF)

                    @pl.when(jnp.logical_not(last))
                    def _():
                        next_copy(b, 0).start()
                obuf[lay, rows, :dh] = x1
                xbuf[lay, 0, rows, :] = uf.astype(BF)
                xbuf[lay, 1, rows, :] = ug.astype(BF)
                xbuf[lay, 2, rows, :] = sf.astype(BF)
                xbuf[lay, 3, rows, :] = sg.astype(BF)
                rbuf[lay, 0, rows, :] = jnp.broadcast_to(rf, (ROWS, 128))
                rbuf[lay, 1, rows, :] = jnp.broadcast_to(rg, (ROWS, 128))
                x_copy(lay, b).start()
                r_copy(lay, b).start()
                pair_copy(lay, b).start()
                y1, y2 = x1, x2
            return 0

        lax.fori_loop(0, blocks, act, 0)

    def times_transposed(delta, weight):
        return lax.dot_general(delta, weight, (((1,), (1,)), ((), ())), preferred_element_type=F32)

    @pl.when(core == 0)
    def _():
        def grad(b, _):
            rows = rows_of(b)
            for part in (0, 1):
                cols = pl.ds(part * dh, dh)
                arrived(rgrad.at[rows, cols], s_rgrad.at[b, part])
            gy1 = rgrad[rows, :dh].astype(F32)
            gy2 = rgrad[rows, dh:].astype(F32)
            for lay in (1, 0):
                arrived(xbuf.at[lay, :, rows, :], r_x.at[lay, b])
                arrived(rbuf.at[lay, :, rows, :], r_r.at[lay, b])
                cf, cg = gain[lay, 0:1, :], gain[lay, 1:2, :]
                uf, ug = xbuf[lay, 0, rows, :].astype(F32), xbuf[lay, 1, rows, :].astype(F32)
                sf, sg = xbuf[lay, 2, rows, :].astype(F32), xbuf[lay, 3, rows, :].astype(F32)
                rf, rg = rbuf[lay, 0, rows, 0:1], rbuf[lay, 1, rows, 0:1]
                delta = (gy2 * sg).astype(BF)
                dbuf[lay, 1, rows, :] = delta
                back = times_transposed(delta, W[lay, 1])
                gacc[lay, 1] += back * ug
                w = cg * back
                gz = gy1 + rg * (w - ug * jnp.mean(w * ug, axis=-1, keepdims=True))
                gbuf[lay, rows, :dh] = gz.astype(BF)
                if lay == 0:
                    @pl.when(jnp.logical_not(last))
                    def _():
                        gnext_copy(b, 0).start()
                delta = (gz * sf).astype(BF)
                dbuf[lay, 0, rows, :] = delta
                back = times_transposed(delta, W[lay, 0])
                gacc[lay, 0] += back * uf
                w = cf * back
                gx = gy2 + rf * (w - uf * jnp.mean(w * uf, axis=-1, keepdims=True))
                gbuf[lay, rows, dh:] = gx.astype(BF)
                if lay == 0:
                    @pl.when(jnp.logical_not(last))
                    def _():
                        gnext_copy(b, 1).start()
                else:
                    d_copy(b).start()
                grad_copy(lay, b).start()
                gy1, gy2 = gz, gx
            return 0

        lax.fori_loop(0, blocks, grad, 0)
        for lay in (0, 1):
            gsum[lay] = jnp.sum(gacc[lay], axis=1)
        remote(gsum.at[1], gsum.at[1], s_gs.at[0], s_gs.at[1], partner).start()

    @pl.when(core == 1)
    def _():
        def wait_d(b, _):
            arrived(dbuf.at[1, :, rows_of(b), :], r_d.at[b])
            return 0
        lax.fori_loop(0, blocks, wait_d, 0)
        arrived(gsum.at[1], s_gs.at[1])

    gmine[...] = gsum[core]
    e_y = remote(gmine, gpeer, es_y.at[0], es_y.at[1], y_peer)
    e_y.start()

    width = min(128, dh)

    def weight_grad(h):
        def outer(i, _):
            at = pl.ds(pl.multiple_of(i * width, width), width)
            normed = (xbuf[core, h, :, at].astype(F32) * gain[core, h, at][None, :]).astype(BF)
            P_[h, at, :] = lax.dot_general(
                normed, dbuf[core, h], (((0,), (0,)), ((), ())), preferred_element_type=F32
            ).astype(BF)
            return 0

        lax.fori_loop(0, dh // width, outer, 0)

    signs, hops = (long_sign, -long_sign), (half, half - 1)
    order = [(d, hops[d] - i) for i in range(half) for d in (0, 1) if i < hops[d]] + [(0, 0)]

    def mine(h, plane, zz):
        return P_.at[h, pl.ds(pl.multiple_of(index_of(plane, zz) * slab, slab), slab), :]

    def f_to_y(zz):
        zz = lax.rem(zz + nz, nz)
        return remote(mine(0, 1 - y, zz), RY.at[zz], qs_y.at[zz], qr_y.at[zz], y_peer)

    def ring(chain, d, i, source):
        return remote(source, RZ.at[chain, d, i], qs_z.at[chain, d, i], qr_z.at[chain, d, i], z_peer(signs[d]))

    def gains_ring(d, i):
        at = gslot.at[lax.rem(z - signs[d] * i + nz, nz)]
        return remote(at, at, es_z.at[d, i], er_z.at[d, i], z_peer(signs[d]))

    weight_grad(0)
    for d, far in order:
        f_to_y(z + signs[d] * far).start()
    weight_grad(1)
    e_y.wait()
    gslot[z] = gmine[...] + gpeer[...]

    def terms(chain, zz):
        h, other = ((1, 0), (1, 1), (0, 0))[chain]
        own = mine(h, y if other == 0 else 1 - y, zz)
        total = own[...].astype(F32)
        if chain == 2:
            zz = lax.rem(zz + nz, nz)
            arrived(RY.at[zz], qr_y.at[zz])
            total = total + RY[zz].astype(F32)
        return own, total

    for i in range(half):
        for d in (0, 1):
            if i < hops[d]:
                if i > 0:
                    arrived(gslot.at[lax.rem(z - signs[d] * i + nz, nz)], er_z.at[d, i - 1])
                gains_ring(d, i).start()
        for chain in (1, 0, 2):
            for d in (0, 1):
                if i >= hops[d]:
                    continue
                far = z + signs[d] * (hops[d] - i)
                if i > 0:
                    arrived(RZ.at[chain, d, i - 1], qr_z.at[chain, d, i - 1])
                own, total = terms(chain, far)
                if i > 0:
                    source = RZ.at[chain, d, i - 1]
                    source[...] = (total + source[...].astype(F32)).astype(BF)
                else:
                    source = own
                    if chain == 2:
                        source[...] = total.astype(BF)
                ring(chain, d, i, source).start()

    def total_of(chain):
        for d in (0, 1):
            if hops[d] > 0:
                arrived(RZ.at[chain, d, hops[d] - 1], qr_z.at[chain, d, hops[d] - 1])
        _, total = terms(chain, z)
        for d in (0, 1):
            if hops[d] > 0:
                total = total + RZ[chain, d, hops[d] - 1].astype(F32)
        return total

    YG[...] = total_of(1).astype(BF)
    g_to_y = remote(YG, RY.at[nz], qs_y.at[nz], qr_y.at[nz], y_peer)
    g_to_y.start()
    g_out[0] = total_of(0)
    f_out[0] = total_of(2)
    for d in (0, 1):
        if hops[d] > 0:
            arrived(gslot.at[lax.rem(z - signs[d] * hops[d] + nz, nz)], er_z.at[d, hops[d] - 1])
    gain_total = gslot[0]
    for zz in range(1, nz):
        gain_total = gain_total + gslot[zz]
    gain_out[0] = gain_total
    arrived(RY.at[nz], qr_y.at[nz])
    g_out[0] = g_out[0] + RY[nz].astype(F32)
    g_to_y.wait_send()
    for zz in range(nz):
        f_to_y(z + zz).wait_send()
    for d in (0, 1):
        for i in range(hops[d]):
            gains_ring(d, i).wait_send()
            for chain in (0, 1, 2):
                ring(chain, d, i, RZ.at[chain, d, i]).wait_send()

    @pl.when(core == 1)
    def _():
        def done(b, _):
            for lay in (0, 1):
                x_copy(lay, b).wait_send()
                r_copy(lay, b).wait_send()
                sent(pair_copy(lay, b), lay == 1)
            arrived(grad_out.at[0, rows_of(b), :], r_grad.at[b])

            @pl.when(jnp.logical_not(last))
            def _():
                next_copy(b, 0).wait_send()
                next_copy(b, 1).wait_send()
            return 0
        lax.fori_loop(0, blocks, done, 0)

    @pl.when(core == 0)
    def _():
        def done(b, _):
            d_copy(b).wait_send()
            for lay in (0, 1):
                sent(grad_copy(lay, b), lay == 0)
            arrived(pair_out.at[0, rows_of(b), :], r_pair.at[b])

            @pl.when(jnp.logical_not(last))
            def _():
                gnext_copy(b, 0).wait_send()
                gnext_copy(b, 1).wait_send()
            return 0
        lax.fori_loop(0, blocks, done, 0)
        remote(gsum.at[1], gsum.at[1], s_gs.at[0], s_gs.at[1], partner).wait_send()

    gain_copy.wait_send()
    to_y(1, dp).wait_send()

    def y_done(zz, _):
        to_y(0, index_of(y, zz)).wait_send()
        return 0
    lax.fori_loop(0, nz, y_done, 0)

    def peer_done(index, _):
        to_peer(0, index).wait_send()
        to_peer(1, index).wait_send()
        return 0
    lax.fori_loop(0, n_dp, peer_done, 0)
    for chain in (0, 1, 2):
        for step in range(half):
            for copy in sends(chain, step):
                copy.wait_send()


def shards(n_section, n_dp, out_pair, out_grad, f_weight, g_weight, gains):
    tok, width = out_pair.shape
    dh = width // 2
    slab = f_weight.shape[1]
    blocks = tok // ROWS
    nz = n_dp // NY
    half = nz // 2
    any_space = pl.BlockSpec(memory_space=pl.ANY)
    vmem = pl.BlockSpec(memory_space=pltpu.VMEM)
    dma = pltpu.SemaphoreType.DMA
    return pl.pallas_call(
        functools.partial(relay_kernel, n_section, n_dp),
        out_shape=(
            jax.ShapeDtypeStruct((1, tok, width), F32),
            jax.ShapeDtypeStruct((1, tok, width), BF),
            jax.ShapeDtypeStruct((1, slab, dh), F32),
            jax.ShapeDtypeStruct((1, slab, dh), F32),
            jax.ShapeDtypeStruct((1, 2, dh), F32),
        ),
        in_specs=[any_space] * 5,
        out_specs=(any_space, any_space, vmem, vmem, vmem),
        scratch_shapes=[
            pltpu.VMEM((2, 2, dh, dh), BF),
            pltpu.VMEM((2, 2, dh), F32),
            pltpu.VMEM((tok, width), BF),
            pltpu.VMEM((tok, width), BF),
            pltpu.VMEM((tok, width), BF),
            pltpu.VMEM((2, tok, width), F32),
            pltpu.VMEM((2, 4, tok, dh), BF),
            pltpu.VMEM((2, 2, tok, 128), F32),
            pltpu.VMEM((2, 2, tok, dh), BF),
            pltpu.VMEM((2, tok, width), BF),
            pltpu.VMEM((2, 2, ROWS, dh), F32),
            pltpu.VMEM((2, 2, dh), F32),
            pltpu.VMEM((2, dh, dh), BF),
            pltpu.VMEM((3, 2, half, slab, dh), BF),
            pltpu.VMEM((nz + 1, slab, dh), BF),
            pltpu.VMEM((slab, dh), BF),
            pltpu.VMEM((nz, 2, dh), F32),
            pltpu.VMEM((2, dh), F32),
            pltpu.VMEM((2, dh), F32),
            dma((4,)), dma((2, n_dp)), dma((2, n_dp)), dma((2, n_dp)), dma((2, n_dp)), dma((3, 2, half)), dma((2,)),
            dma((blocks, 2)), dma((blocks, 2)), dma((blocks, 2)), dma((blocks, 2)),
            dma((2, blocks)), dma((2, blocks)), dma((2, blocks)), dma((2, blocks)),
            dma((2, blocks)), dma((blocks,)), dma((blocks,)), dma((blocks,)), dma((2, blocks)), dma((blocks,)), dma((2,)),
            dma((3, 2, half)), dma((3, 2, half)), dma((nz + 1,)), dma((nz + 1,)), dma((2, half)), dma((2, half)), dma((2,)),
        ],
        compiler_params=pltpu.CompilerParams(
            collective_id=0, has_side_effects=True, vmem_limit_bytes=60 * 1024 * 1024
        ),
        name="relay",
    )(out_pair, out_grad, f_weight, g_weight, gains)


def solution(mesh):
    sizes = dict(mesh.shape)
    return jax.shard_map(
        functools.partial(shards, sizes["section"], sizes["dp"]),
        mesh=mesh,
        in_specs=(P("dp", None), P("dp", None), P("section", "dp", None), P("section", "dp", None), P("section", None, None)),
        out_specs=(
            P("section", "dp", None),
            P("section", "dp", None),
            P("section", "dp", None),
            P("section", "dp", None),
            P("section", None, None),
        ),
        check_vma=False,
    )
```
